32 devices in a mesh: row: 16 (over z, y, core), rows: 2 (over x).
Axes of the slice: x: 2, y: 2, z: 4, core: 2. Of those that a mesh axis runs over, the one named last changes fastest.
Arguments:
- hopping: float32 [2, 128, 512, 512], P(None, 'row', 'rows'), may hold values from -0.5 to 0.5
- lattice: int32 [3, 128], replicated, may hold values from -4 to 4
- kgrid: int32 [3, 32], replicated, may hold values from 0 to 7
- tangent: float32 [3, 32], replicated, may hold values from -4 to 4
- states: float32 [2, 32, 1024, 512], P(None, 'row'), may hold values from -6 to 6
Outputs:
- energies: float32 [32, 1024], P('row')
- velocities: float32 [32, 1024], P('row')
The draws below stay inside these ranges and needn't reach their ends.
All inputs are finite; a program needn't handle non-finite values.
Results may differ from the reference program's by a relative error of at most 0.000075.
Values sent between devices are 32-bit elements; how exact they have to be, the bound alone decides.
A program may use at most 256 MiB of HBM per device.

```python
import math
import jax
import jax.numpy as jnp
from jax import lax

NW = 512
NR = 128
NB = 1024
K = 32
KGRID = 8


def with_ends(result, rng, smallest, high):
    dims = result.shape
    place = [jax.random.randint(jax.random.fold_in(rng, axis), (), 0, dims[axis]) for axis in range(len(dims))]
    result = result.at[tuple(place)].set(smallest)
    longest = dims.index(max(dims))
    place[longest] = (place[longest] + 1) % dims[longest]
    return result.at[tuple(place)].set(high)


def level_of(key, dims, cuts, least, high):
    factor_of, own = 1.0, jax.random.fold_in(key, 6)
    for dim, parts in cuts:
        steps = jnp.exp(jax.random.uniform(jax.random.fold_in(own, dim), (parts,), jnp.float32, least / len(cuts), high / len(cuts)))
        factor_of = factor_of * jnp.repeat(steps, dims[dim] // parts).reshape([-1 if axis == dim else 1 for axis in range(len(dims))])
    return factor_of


def scatter_about(stream_key, shape, spread, bound, pieces=(), held_as=jnp.bfloat16):
    factor_of = level_of(stream_key, shape, pieces, -0.22, 0.18) if pieces else 1.0
    values = jax.random.normal(stream_key, shape, jnp.float32) * spread * factor_of
    return jnp.minimum(jnp.maximum(values, -bound), bound).astype(held_as)


def setup_inputs(seed: int = 0) -> dict:
    splits = jax.random.split(jax.random.key(seed), 6)
    hopping = scatter_about(splits[0], (2, NR, NW, NW), NR ** -0.5, 0.5, ((1, 16), (2, 2)), jnp.float32)
    lattice = with_ends(jax.random.randint(splits[1], (3, NR), -4, 5), jax.random.fold_in(splits[1], 1), -4, 4).astype(jnp.int32)
    kgrid = with_ends(jax.random.randint(splits[2], (3, K), 0, KGRID), jax.random.fold_in(splits[2], 1), 0, KGRID - 1).astype(jnp.int32)
    tangent = scatter_about(splits[3], (3, K), 0.3, 4.0, (), jnp.float32)
    states = scatter_about(splits[4], (2, K, NB, NW), 1.0, 6.0, ((1, 16),), jnp.float32)
    return {"hopping": hopping, "lattice": lattice, "kgrid": kgrid, "tangent": tangent, "states": states}


def phases(kgrid, lattice, tangent):
    turns = jnp.mod(jnp.sum(kgrid[:, :, None] * lattice[:, None, :], axis=0), KGRID)
    angle = turns.astype(jnp.float32) * (2.0 * math.pi / KGRID)
    weight = jnp.sum(tangent[:, :, None] * lattice[:, None, :].astype(jnp.float32), axis=0)
    return jnp.cos(angle), jnp.sin(angle), weight


def expand(first, second, hopping):
    real_sum = jnp.einsum("kr,rab->kab", first, hopping[0], precision=lax.Precision.HIGHEST)
    imag_sum = jnp.einsum("kr,rab->kab", second, hopping[1], precision=lax.Precision.HIGHEST)
    cross_one = jnp.einsum("kr,rab->kab", second, hopping[0], precision=lax.Precision.HIGHEST)
    cross_two = jnp.einsum("kr,rab->kab", first, hopping[1], precision=lax.Precision.HIGHEST)
    return real_sum - imag_sum, cross_one + cross_two


def project(m_re, m_im, rows, cols):
    high = lax.Precision.HIGHEST
    y_re = jnp.einsum("kac,kic->kai", m_re, cols[0], precision=high) - jnp.einsum("kac,kic->kai", m_im, cols[1], precision=high)
    y_im = jnp.einsum("kac,kic->kai", m_re, cols[1], precision=high) + jnp.einsum("kac,kic->kai", m_im, cols[0], precision=high)
    return jnp.einsum("kia,kai->ki", rows[0], y_re, precision=high) + jnp.einsum("kia,kai->ki", rows[1], y_im, precision=high)


def reference(hopping, lattice, kgrid, tangent, states):
    cosine, sine, weight = phases(kgrid, lattice, tangent)
    hk_re, hk_im = expand(cosine, sine, hopping)
    dk_re, dk_im = expand(-weight * sine, weight * cosine, hopping)
    p_h = project(hk_re, hk_im, states, states)
    p_d = project(dk_re, dk_im, states, states)
    norm = jnp.sum(states[0] * states[0] + states[1] * states[1], axis=-1)
    return p_h / norm, p_d / norm
```

```python
import functools
import math

import jax
import jax.numpy as jnp
from jax import lax
from jax.experimental import pallas as pl
from jax.experimental.pallas import tpu as pltpu
from jax.sharding import PartitionSpec as P

KGRID = 8
LINE = 4
LANES = 128
SUB = 16
MESH = pl.DeviceIdType.MESH
F32 = jnp.float32
BF16 = jnp.bfloat16


def phases(kgrid, lattice, tangent):
    turns = jnp.mod(jnp.sum(kgrid[:, :, None] * lattice[:, None, :], axis=0), KGRID)
    angle = turns.astype(jnp.float32) * (2.0 * math.pi / KGRID)
    weight = jnp.sum(tangent[:, :, None] * lattice[:, None, :].astype(jnp.float32), axis=0)
    return (jnp.cos(angle), jnp.sin(angle), weight)


def split(value):
    high = value.astype(BF16)
    return high, (value - high.astype(F32)).astype(BF16)


def coefficients(lattice, kgrid, tangent, group, per):
    place = lax.axis_index("row") // group
    count = group * per
    mine = lax.dynamic_slice_in_dim(lattice, place * count, count, 1)
    cosine, sine, weight = (v.reshape(-1, group, 1, per) for v in phases(kgrid, mine, tangent))
    plus, minus = 0.5 * (cosine + sine), 0.5 * (cosine - sine)
    energy = jnp.concatenate([plus, minus], axis=2)
    slope = weight * jnp.concatenate([minus, -plus], axis=2)
    coef = jnp.stack([energy, slope], axis=1)
    coef = coef.reshape(LINE, -1, 2 * count)
    coef = jnp.where(place < LINE // 2, coef, coef[::-1])
    return coef.reshape(-1, 2 * count)


def kernel(
    dims,
    coef_ref,
    hop,
    states,
    energy_ref,
    slope_ref,
    coef3,
    hown,
    ht,
    uvs,
    uva,
    part,
    got1,
    got2,
    tk,
    st,
    wide,
    fine,
    acc,
    sums,
    hsem,
    tsem,
    ssem,
    xs,
    xr,
    gs,
    gr,
    s1,
    r1,
    s2,
    r2,
    s3,
    r3,
    ds,
    dr,
    es,
    er,
):
    X, G, per, nb, kd, NB = dims
    nbc = nb // LANES
    nch = X * nbc
    span = G * SUB
    nsub = nb // span
    nt = nch * nsub
    kb = part.shape[2]
    slots = st.shape[0]
    row, x = lax.axis_index("row"), lax.axis_index("rows")
    a, g = row // G, lax.rem(row, G)
    outer = (a == 0) | (a == LINE - 1)
    inner = jnp.logical_not(outer)
    beside = a + 1 - 2 * lax.rem(a, 2)
    across = LINE - 1 - a
    own = jnp.where(outer, 0, 1)

    def column(j):
        home = lax.rem(x + j // nbc, X)
        return pl.multiple_of(home * nb + lax.rem(j, nbc) * LANES, LANES)

    def at(position, member):
        return {"row": position * G + member, "rows": x}

    def remote(src, dst, send, recv, device):
        return pltpu.make_async_remote_copy(
            src_ref=src, dst_ref=dst, send_sem=send, recv_sem=recv, device_id=device, device_id_type=MESH
        )

    def load_own(j):
        slot = lax.rem(j, 2)
        return pltpu.make_async_copy(hop.at[:, :, :, pl.ds(column(j), LANES)], hown.at[slot], hsem.at[slot])

    def load_turned(j):
        start = pl.multiple_of(x * nb, LANES)
        return pltpu.make_async_copy(
            hop.at[:, :, pl.ds(j * LANES, LANES), pl.ds(start, nb)], ht.at[j], tsem.at[j]
        )

    def load_states(j):
        slot = lax.rem(j, slots)
        return pltpu.make_async_copy(states.at[:, :, :, pl.ds(column(j), LANES)], st.at[slot], ssem.at[slot])

    def turned_copy(o, q):
        to = lax.rem(x - o + X, X)
        start = pl.multiple_of(to * nb, LANES)
        n = (o - 1) * nbc + q
        return remote(
            hop.at[:, :, pl.ds(q * LANES, LANES), pl.ds(start, nb)],
            ht.at[o * nbc + q],
            xs.at[n],
            xr.at[n],
            {"row": row, "rows": to},
        )

    def turned_arrival(j):
        return remote(ht.at[j], ht.at[j], xs.at[j - nbc], xr.at[j - nbc], {"row": row, "rows": lax.rem(x + 1, X)})

    def share_copy(t, o):
        to = lax.rem(g + o, G)
        return remote(uvs.at[t, to], uva.at[t, g], gs.at[t, o - 1], gr.at[t, o - 1], at(a, to))

    def share_arrival(t, o):
        source = lax.rem(g - o + G, G)
        return remote(uvs.at[t, source], uva.at[t, source], gs.at[t, o - 1], gr.at[t, o - 1], at(a, source))

    def first_copy(t):
        return remote(part.at[t, pl.ds(1, 3)], got1.at[t], s1.at[t], r1.at[t], at(beside, g))

    def second_copy(t):
        return remote(part.at[t, pl.ds(2, 2)], got2.at[t], s2.at[t], r2.at[t], at(across, g))

    def third_copy(t):
        return remote(part.at[t, 0], got1.at[t, 0], s3.at[t], r3.at[t], at(beside, g))

    def place_of(t, member):
        return pl.multiple_of(lax.rem(t, nsub) * span + member * SUB, SUB)

    def deal_copy(t, o):
        to = lax.rem(g + o, G)
        return remote(
            part.at[t, own, pl.ds(to * 2 * kd, 2 * kd)],
            tk.at[t // nsub, :, pl.ds(place_of(t, g), SUB), :],
            ds.at[t, o - 1],
            dr.at[t, o - 1],
            at(a, to),
        )

    def deal_arrival(t, o):
        source = lax.rem(g - o + G, G)
        there = tk.at[t // nsub, :, pl.ds(place_of(t, source), SUB), :]
        return remote(there, there, ds.at[t, o - 1], dr.at[t, o - 1], at(a, source))

    for j in range(nbc):
        load_turned(j).start()
    for j in range(2):
        load_own(j).start()
    for j in range(slots):
        load_states(j).start()

    barrier = pltpu.get_barrier_semaphore()
    for o in range(1, X):
        pl.semaphore_signal(barrier, inc=1, device_id={"row": row, "rows": lax.rem(x + o, X)}, device_id_type=MESH)
    for o in range(1, G):
        pl.semaphore_signal(barrier, inc=1, device_id=at(a, lax.rem(g + o, G)), device_id_type=MESH)
    for o in range(1, LINE):
        pl.semaphore_signal(barrier, inc=1, device_id=at(lax.rem(a + o, LINE), g), device_id_type=MESH)
    pl.semaphore_wait(barrier, X + G + LINE - 3)

    for q in range(nbc):
        for o in range(1, X):
            turned_copy(o, q).start()

    high, low = split(coef_ref[...])
    coef3[...] = jnp.concatenate([high, high, low], axis=1)

    def produce(j):
        slot = lax.rem(j, 2)
        load_own(j).wait()

        def one(r, carry):
            for h in range(nbc):
                rows = pl.ds(h * LANES, LANES)
                u = hown[slot, 0, r, rows, :] - ht[j, 1, r, :, rows].T
                v = ht[j, 0, r, :, rows].T + hown[slot, 1, r, rows, :]
                for q in range(LANES // SUB):
                    start = h * LANES + q * SUB
                    t, member = j * nsub + start // span, start % span // SUB
                    uvs[t, member, r] = u[q * SUB : (q + 1) * SUB]
                    uvs[t, member, per + r] = v[q * SUB : (q + 1) * SUB]
            return carry

        lax.fori_loop(0, per, one, 0)

        def send(s, carry):
            t = j * nsub + s
            for o in range(1, G):
                share_copy(t, o).start()
            uva[t, g] = uvs[t, g]
            return carry

        lax.fori_loop(0, nsub, send, 0)

    def reload(j):
        @pl.when(j < nch)
        def _():
            load_own(j).start()

    def expand(t):
        for o in range(1, G):
            share_arrival(t, o).wait_recv()
        for h in range(SUB // 8):
            rows = pl.ds(h * 8, 8)
            data = uva[t, :, :, rows, :].reshape(G * 2 * per, 8, LANES)
            data = jnp.swapaxes(data, 0, 1)
            done = []
            for i in range(0, 8, 2):
                high, low = split(jnp.concatenate([data[i], data[i + 1]], axis=1))
                both = jnp.concatenate([high, low, high], axis=0)
                out = jnp.dot(coef3[...], both, preferred_element_type=F32)
                done += [out[:, :LANES], out[:, LANES:]]
            done = jnp.swapaxes(jnp.stack(done), 0, 1)
            part[t, :, :, rows, :] = done.reshape(LINE, kb, 8, LANES)

        @pl.when(outer)
        def _():
            first_copy(t).start()

    def deal(t):
        for o in range(1, G):
            deal_copy(t, o).start()
        tk[t // nsub, :, pl.ds(place_of(t, g), SUB), :] = part[t, own, pl.ds(g * 2 * kd, 2 * kd)]

    def join_first(t):
        first_copy(t).wait_recv()
        part[t, 1:4] += got1[t]
        second_copy(t).start()

    def join_second(t):
        second_copy(t).wait_recv()
        part[t, 0] += got2[t, 1]
        third_copy(t).start()
        part[t, 1] += got2[t, 0]
        deal(t)

    def join_third(t):
        third_copy(t).wait_recv()
        part[t, 0] += got1[t, 0]
        deal(t)

    def project(j):
        def arrived(s, carry):
            for o in range(1, G):
                deal_arrival(j * nsub + s, o).wait_recv()
            return carry

        lax.fori_loop(0, nsub, arrived, 0)
        slot = lax.rem(j, slots)

        @pl.when(j >= slots)
        def _():
            load_states(j).wait()

        rows_at_once = 256
        for k in range(kd):
            high, low = split(jnp.concatenate([tk[j, 2 * k], tk[j, 2 * k + 1]], axis=1))

            def bands(b, carry):
                rows = pl.ds(pl.multiple_of(b * rows_at_once, rows_at_once), rows_at_once)

                def times(side):
                    big, small = wide[k, side, rows, :], fine[k, side, rows, :]
                    return (
                        jnp.dot(big, high, preferred_element_type=F32)
                        + jnp.dot(big, low, preferred_element_type=F32)
                        + jnp.dot(small, high, preferred_element_type=F32)
                    )

                left, right = st[slot, 0, k, rows, :], st[slot, 1, k, rows, :]
                minus, plus = left - right, left + right
                over, under = times(0), times(1)
                acc[k, 0, rows, :] += over[:, :LANES] * minus + under[:, :LANES] * plus
                acc[k, 1, rows, :] += over[:, LANES:] * minus + under[:, LANES:] * plus
                return carry

            lax.fori_loop(0, NB // rows_at_once, bands, 0)

        @pl.when(j + slots < nch)
        def _():
            load_states(j + slots).start()

    def to_row(value):
        return jnp.sum(value.T, axis=0, keepdims=True)

    def prepare():
        for j in range(slots):
            load_states(j).wait()
        for k in range(kd):

            def bands(b, carry):
                rows = pl.ds(pl.multiple_of(b * LANES, LANES), LANES)
                total = jnp.zeros((LANES, LANES), F32)
                for q in range(nbc):
                    for side in range(2):
                        value = st[q, side, k, rows, :]
                        high, low = split(value)
                        wide[k, side, rows, q * LANES : (q + 1) * LANES] = high
                        fine[k, side, rows, q * LANES : (q + 1) * LANES] = low
                        total = total + value * value
                acc[k, 0, rows, :] = jnp.zeros((LANES, LANES), F32)
                acc[k, 1, rows, :] = jnp.zeros((LANES, LANES), F32)
                sums[x, pl.ds(2 * kd + k, 1), rows] = to_row(total)
                return carry

            lax.fori_loop(0, NB // LANES, bands, 0)

    for j in range(nbc):
        load_turned(j).wait()
        produce(j)
        reload(j + 2)
    prepare()

    lag = 5

    def step(t, carry):
        @pl.when(t < nt)
        def _():
            expand(t)

        @pl.when(inner & (t >= 1) & (t - 1 < nt))
        def _():
            join_first(t - 1)

        @pl.when(inner & (t >= 2) & (t - 2 < nt))
        def _():
            join_second(t - 2)

        @pl.when(outer & (t >= 4) & (t - 4 < nt))
        def _():
            join_third(t - 4)

        j = t // nsub + 1

        @pl.when((lax.rem(t, nsub) == nsub - 1) & (j >= nbc) & (j < nch))
        def _():
            turned_arrival(j).wait_recv()
            produce(j)
            reload(j + 2)

        done = t - lag

        @pl.when((done >= 0) & (lax.rem(done + nsub, nsub) == nsub - 1))
        def _():
            project(done // nsub)

        return carry

    lax.fori_loop(0, nt + lag, step, 0)

    for k in range(kd):
        for m in range(2):

            def bands(b, carry):
                rows = pl.ds(pl.multiple_of(b * LANES, LANES), LANES)
                sums[x, pl.ds(2 * k + m, 1), rows] = to_row(acc[k, m, rows, :])
                return carry

            lax.fori_loop(0, NB // LANES, bands, 0)

    def sum_copy(o):
        to = lax.rem(x + o, X)
        return remote(sums.at[x], sums.at[x], es.at[o - 1], er.at[o - 1], {"row": row, "rows": to})

    def sum_arrival(o):
        source = lax.rem(x - o + X, X)
        return remote(sums.at[source], sums.at[source], es.at[o - 1], er.at[o - 1], {"row": row, "rows": source})

    for o in range(1, X):
        sum_copy(o).start()
    for o in range(1, X):
        sum_arrival(o).wait_recv()
    total = sums[0]
    for o in range(1, X):
        total = total + sums[o]
    for k in range(kd):
        norm = total[2 * kd + k : 2 * kd + k + 1]
        energy_ref[k : k + 1, :] = total[2 * k : 2 * k + 1] / norm
        slope_ref[k : k + 1, :] = total[2 * k + 1 : 2 * k + 2] / norm

    for q in range(nbc):
        for o in range(1, X):
            turned_copy(o, q).wait_send()
    for o in range(1, X):
        sum_copy(o).wait_send()

    def settle(t, carry):
        for o in range(1, G):
            share_copy(t, o).wait_send()
            deal_copy(t, o).wait_send()

        @pl.when(outer)
        def _():
            first_copy(t).wait_send()

        @pl.when(inner)
        def _():
            second_copy(t).wait_send()
            third_copy(t).wait_send()

        return carry

    lax.fori_loop(0, nt, settle, 0)


def fits(row, X, hopping, states):
    per, nb, columns = hopping.shape[1:]
    kd, bands = states.shape[1:3]
    if row % LINE or nb % LANES or X < 2 or columns != X * nb:
        return False
    group = row // LINE
    nbc, span = nb // LANES, group * SUB
    return group > 1 and nbc >= 2 and nb % span == 0 and (span <= LANES or span % LANES == 0) and bands % 256 == 0


def one_kernel(hopping, lattice, kgrid, tangent, states):
    X, G = lax.axis_size("rows"), lax.axis_size("row") // LINE
    per, nb = hopping.shape[1:3]
    kd, NB = states.shape[1:3]
    nbc = nb // LANES
    nch = X * nbc
    nt = nch * nb // (G * SUB)
    coef = coefficients(lattice, kgrid, tangent, G, per)
    kb = coef.shape[0] // LINE
    cols = coef.shape[1]
    slots = nbc
    tile = (SUB, LANES)
    dma = pltpu.SemaphoreType.DMA
    out = jax.ShapeDtypeStruct((kd, NB), F32)
    vmem = pl.BlockSpec(memory_space=pltpu.VMEM)
    hbm = pl.BlockSpec(memory_space=pl.ANY)
    rows_of_sums = -(-3 * kd // 8) * 8
    return pl.pallas_call(
        functools.partial(kernel, (X, G, per, nb, kd, NB)),
        out_shape=(out, out),
        in_specs=[vmem, hbm, hbm],
        out_specs=(vmem, vmem),
        scratch_shapes=[
            pltpu.VMEM((LINE * kb, 3 * cols), BF16),
            pltpu.VMEM((2, 2, per, nb, LANES), F32),
            pltpu.VMEM((nch, 2, per, LANES, nb), F32),
            pltpu.VMEM((nt, G, 2 * per, *tile), F32),
            pltpu.VMEM((nt, G, 2 * per, *tile), F32),
            pltpu.VMEM((nt, LINE, kb, *tile), F32),
            pltpu.VMEM((nt, LINE - 1, kb, *tile), F32),
            pltpu.VMEM((nt, LINE // 2, kb, *tile), F32),
            pltpu.VMEM((nch, 2 * kd, nb, LANES), F32),
            pltpu.VMEM((slots, 2, kd, NB, LANES), F32),
            pltpu.VMEM((kd, 2, NB, nb), BF16),
            pltpu.VMEM((kd, 2, NB, nb), BF16),
            pltpu.VMEM((kd, 2, NB, LANES), F32),
            pltpu.VMEM((X, rows_of_sums, NB), F32),
            dma((2,)),
            dma((nbc,)),
            dma((slots,)),
            dma(((X - 1) * nbc,)),
            dma(((X - 1) * nbc,)),
            dma((nt, G - 1)),
            dma((nt, G - 1)),
            dma((nt,)),
            dma((nt,)),
            dma((nt,)),
            dma((nt,)),
            dma((nt,)),
            dma((nt,)),
            dma((nt, G - 1)),
            dma((nt, G - 1)),
            dma((X - 1,)),
            dma((X - 1,)),
        ],
        compiler_params=pltpu.CompilerParams(
            collective_id=0, has_side_effects=True, vmem_limit_bytes=67043328
        ),
    )(coef, hopping, states)


def project(m_re, m_im, rows, cols):
    high = lax.Precision.HIGH
    y_re = jnp.einsum("kmac,kic->kmai", m_re, cols[0], precision=high) - jnp.einsum(
        "kmac,kic->kmai", m_im, cols[1], precision=high
    )
    y_im = jnp.einsum("kmac,kic->kmai", m_re, cols[1], precision=high) + jnp.einsum(
        "kmac,kic->kmai", m_im, cols[0], precision=high
    )
    a = jnp.swapaxes(rows[0], 1, 2)[:, None]
    b = jnp.swapaxes(rows[1], 1, 2)[:, None]
    return jnp.sum(a * y_re + b * y_im, axis=2)


def exchanges(hopping, lattice, kgrid, tangent, states):
    row_count = hopping.shape[2]
    row_start = lax.axis_index("rows") * row_count
    state_rows = lax.dynamic_slice_in_dim(states, row_start, row_count, 3)
    cosine, sine, weight = phases(kgrid, lattice, tangent)
    first_d, second_d = -weight * sine, weight * cosine
    coef = jnp.stack(
        [
            jnp.stack([cosine, -sine], axis=1),
            jnp.stack([sine, cosine], axis=1),
            jnp.stack([first_d, -second_d], axis=1),
            jnp.stack([second_d, first_d], axis=1),
        ],
        axis=1,
    )
    halves = 2 if row_count % (2 * lax.axis_size("row")) == 0 else 1
    part = row_count // halves
    slabs = [
        lax.all_to_all(hopping[:, :, h * part : (h + 1) * part], "row", 2, 1, tiled=True)
        for h in range(halves)
    ]
    tiles = []
    for slab in slabs:
        blocks = jnp.einsum("kmpr,prac->kmac", coef, slab, precision=lax.Precision.HIGHEST)
        tiles.append(lax.all_to_all(blocks, "row", 0, 2, tiled=True))
    pieces = 0.0
    for h, tile in enumerate(tiles):
        rows = state_rows[..., h * part : (h + 1) * part]
        pieces = pieces + project(tile[:, 0::2], tile[:, 1::2], rows, states)
    totals = lax.psum(pieces, "rows")
    norm = jnp.sum(states[0] * states[0] + states[1] * states[1], axis=-1)
    return (totals[:, 0] / norm, totals[:, 1] / norm)


def per_device(hopping, lattice, kgrid, tangent, states):
    if fits(lax.axis_size("row"), lax.axis_size("rows"), hopping, states):
        return one_kernel(hopping, lattice, kgrid, tangent, states)
    return exchanges(hopping, lattice, kgrid, tangent, states)


def solution(mesh):
    placed = (P(None, "row", "rows", None), P(), P(), P(), P(None, "row", None, None))
    return jax.shard_map(
        per_device,
        mesh=mesh,
        in_specs=placed,
        out_specs=(P("row", None), P("row", None)),
        check_vma=False,
    )
```

```python
import functools
import math

import jax
import jax.numpy as jnp
from jax import lax
from jax.experimental import pallas as pl
from jax.experimental.pallas import tpu as pltpu
from jax.sharding import PartitionSpec as P

KGRID = 8
AHEAD = 2
FLIGHT = 2
LAGS = (1, 3, 8)
SHIFT = 1
LINE = 4
LANES = 128
SUB = 8
MESH = pl.DeviceIdType.MESH
F32 = jnp.float32
BF16 = jnp.bfloat16


def split(value):
    high = value.astype(BF16)
    return high, (value - high.astype(F32)).astype(BF16)


def coefficients(lattice, kgrid, tangent, place, shape, per):
    exact = lax.Precision.HIGHEST
    block = shape[0] // LINE
    count = shape[1] // 2

    def iota(dims, axis):
        return lax.broadcasted_iota(jnp.int32, dims, axis)

    row = iota((shape[0], kgrid.shape[1]), 0)
    home = lax.div(row, block)
    home = jnp.where(place < LINE // 2, home, LINE - 1 - home)
    which = home * (block // 2) + lax.div(lax.rem(row, block), 2)
    pick_k = (which == iota(row.shape, 1)).astype(F32)
    column = iota((lattice.shape[1], shape[1]), 1)
    which = place * count + lax.div(column, 2 * per) * per + lax.rem(column, per)
    pick_r = (which == iota(column.shape, 0)).astype(F32)
    far = jnp.dot(lattice.astype(F32), pick_r, precision=exact, preferred_element_type=F32)

    def near(value):
        return lax.dot_general(pick_k, value, (((1,), (1,)), ((), ())), precision=exact, preferred_element_type=F32)

    def inner(left):
        return left[:, 0:1] * far[0:1] + left[:, 1:2] * far[1:2] + left[:, 2:3] * far[2:3]

    turns = inner(near(kgrid.astype(F32))).astype(jnp.int32) & (KGRID - 1)
    weight = inner(near(tangent))

    def wave(turn):
        turn = turn & (KGRID - 1)
        turn = jnp.minimum(turn, KGRID - turn)
        value = jnp.full(shape, -1.0, F32)
        for step in range(KGRID // 2):
            value = jnp.where(turn == step, F32(math.cos(2.0 * math.pi * step / KGRID)), value)
        return value

    cosine, sine = wave(turns), wave(turns - KGRID // 4)
    plus, minus = 0.5 * (cosine + sine), 0.5 * (cosine - sine)
    second = lax.rem(lax.div(iota(shape, 1), per), 2) == 1
    slope = lax.rem(iota(shape, 0), 2) == 1
    return jnp.where(slope, weight * jnp.where(second, -plus, minus), jnp.where(second, minus, plus))


def kernel(
    dims,
    lattice_ref,
    kgrid_ref,
    tangent_ref,
    hop,
    states,
    out_ref,
    coef3,
    hown,
    ht,
    uvs,
    uva,
    part,
    got1,
    got2,
    tk,
    st,
    wide,
    fine,
    acc,
    sums,
    hsem,
    tsem,
    ssem,
    xs,
    xr,
    gs,
    gr,
    s1,
    r1,
    s2,
    r2,
    s3,
    r3,
    ds,
    dr,
    es,
    er,
):
    X, G, per, nb, kd, NB = dims
    nbc = nb // LANES
    nch = X * nbc
    span = G * SUB
    nsub = nb // span
    nt = nch * nsub
    ahead, flight = min(AHEAD, nsub), FLIGHT
    kb = part.shape[2]
    slots = st.shape[0]
    row, x = lax.axis_index("row"), lax.axis_index("rows")
    a, g = row // G, lax.rem(row, G)
    outer = (a == 0) | (a == LINE - 1)
    inner = jnp.logical_not(outer)
    beside = a + 1 - 2 * lax.rem(a, 2)
    across = LINE - 1 - a
    own = jnp.where(outer, 0, 1)

    def column(j):
        home = lax.rem(x + j // nbc, X)
        return pl.multiple_of(home * nb + lax.rem(j, nbc) * LANES, LANES)

    def at(position, member):
        return {"row": position * G + member, "rows": x}

    def remote(src, dst, send, recv, device):
        return pltpu.make_async_remote_copy(
            src_ref=src, dst_ref=dst, send_sem=send, recv_sem=recv, device_id=device, device_id_type=MESH
        )

    def load_own(j):
        slot = lax.rem(j, 2)
        return pltpu.make_async_copy(hop.at[:, :, :, pl.ds(column(j), LANES)], hown.at[slot], hsem.at[slot])

    def load_turned(j):
        start = pl.multiple_of(x * nb, LANES)
        return pltpu.make_async_copy(
            hop.at[:, :, pl.ds(j * LANES, LANES), pl.ds(start, nb)], ht.at[j], tsem.at[j]
        )

    def load_states(j):
        slot = lax.rem(j, slots)
        return pltpu.make_async_copy(states.at[:, :, :, pl.ds(column(j), LANES)], st.at[slot], ssem.at[slot])

    def turned_copy(o, q):
        to = lax.rem(x - o + X, X)
        start = pl.multiple_of(to * nb, LANES)
        n = (o - 1) * nbc + q
        return remote(
            hop.at[:, :, pl.ds(q * LANES, LANES), pl.ds(start, nb)],
            ht.at[o * nbc + q],
            xs.at[n],
            xr.at[n],
            {"row": row, "rows": to},
        )

    def turned_arrival(j):
        return remote(ht.at[j], ht.at[j], xs.at[j - nbc], xr.at[j - nbc], {"row": row, "rows": lax.rem(x + 1, X)})

    def share_copy(t, o):
        to = lax.rem(g + o, G)
        return remote(uvs.at[t, to], uva.at[t, g], gs.at[t, o - 1], gr.at[t, o - 1], at(a, to))

    def share_arrival(t, o):
        source = lax.rem(g - o + G, G)
        return remote(uvs.at[t, source], uva.at[t, source], gs.at[t, o - 1], gr.at[t, o - 1], at(a, source))

    def first_copy(t):
        return remote(part.at[t, pl.ds(1, 3)], got1.at[t], s1.at[t], r1.at[t], at(beside, g))

    def second_copy(t):
        return remote(part.at[t, pl.ds(2, 2)], got2.at[t], s2.at[t], r2.at[t], at(across, g))

    def third_copy(t):
        return remote(part.at[t, 0], got1.at[t, 0], s3.at[t], r3.at[t], at(beside, g))

    def place_of(t, member):
        return pl.multiple_of(lax.rem(t, nsub) * span + member * SUB, SUB)

    def deal_copy(t, o):
        to = lax.rem(g + o, G)
        return remote(
            part.at[t, own, pl.ds(to * 2 * kd, 2 * kd)],
            tk.at[t // nsub, :, pl.ds(place_of(t, g), SUB), :],
            ds.at[t, o - 1],
            dr.at[t, o - 1],
            at(a, to),
        )

    def deal_arrival(t, o):
        source = lax.rem(g - o + G, G)
        there = tk.at[t // nsub, :, pl.ds(place_of(t, source), SUB), :]
        return remote(there, there, ds.at[t, o - 1], dr.at[t, o - 1], at(a, source))

    load_turned(0).start()
    load_own(0).start()

    barrier = pltpu.get_barrier_semaphore()
    for o in range(1, X):
        pl.semaphore_signal(barrier, inc=1, device_id={"row": row, "rows": lax.rem(x + o, X)}, device_id_type=MESH)
    for o in range(1, G):
        pl.semaphore_signal(barrier, inc=1, device_id=at(a, lax.rem(g + o, G)), device_id_type=MESH)
    for o in range(1, LINE):
        pl.semaphore_signal(barrier, inc=1, device_id=at(lax.rem(a + o, LINE), g), device_id_type=MESH)
    shape = (coef3.shape[0], coef3.shape[1] // 3)
    high, low = split(coefficients(lattice_ref[...], kgrid_ref[...], tangent_ref[...], a, shape, per))
    coef3[...] = jnp.concatenate([high, high, low], axis=1)

    pl.semaphore_wait(barrier, X + G + LINE - 3)

    for o in range(1, X):
        turned_copy(o, 0).start()
    for j in range(1, nbc):
        load_turned(j).start()
    load_own(1).start()
    for j in range(slots):
        load_states(j).start()


    batch = LANES // span

    def produce(j, h):
        slot = lax.rem(j, 2)
        rows = pl.ds(h * LANES, LANES)
        first = j * nsub + h * batch

        def one(r, carry):
            u = hown[slot, 0, r, rows, :] - ht[j, 1, r, :, rows].T
            v = ht[j, 0, r, :, rows].T + hown[slot, 1, r, rows, :]
            for q in range(LANES // SUB):
                t, member = first + q // G, q % G
                uvs[t, member, r] = u[q * SUB : (q + 1) * SUB]
                uvs[t, member, per + r] = v[q * SUB : (q + 1) * SUB]
            return carry

        lax.fori_loop(0, per, one, 0)

    def share(t):
        for o in range(1, G):
            share_copy(t, o).start()
        uva[t, g] = uvs[t, g]

    def reload(j):
        @pl.when(j < nch)
        def _():
            load_own(j).start()

    def expand(t):
        for o in range(1, G):
            share_arrival(t, o).wait_recv()
        for h in range(SUB // 8):
            rows = pl.ds(h * 8, 8)
            data = uva[t, :, :, rows, :].reshape(G * 2 * per, 8, LANES)
            data = jnp.swapaxes(data, 0, 1)
            done = []
            for i in range(0, 8, 2):
                high, low = split(jnp.concatenate([data[i], data[i + 1]], axis=1))
                both = jnp.concatenate([high, low, high], axis=0)
                out = jnp.dot(coef3[...], both, preferred_element_type=F32)
                done += [out[:, :LANES], out[:, LANES:]]
            done = jnp.swapaxes(jnp.stack(done), 0, 1)
            part[t, :, :, rows, :] = done.reshape(LINE, kb, 8, LANES)

        @pl.when(outer)
        def _():
            @pl.when(t >= flight)
            def _():
                first_copy(t - flight).wait_send()

            first_copy(t).start()

    def deal(t):
        for o in range(1, G):
            deal_copy(t, o).start()
        tk[t // nsub, :, pl.ds(place_of(t, g), SUB), :] = part[t, own, pl.ds(g * 2 * kd, 2 * kd)]

    def join_first(t):
        first_copy(t).wait_recv()
        part[t, 1:4] += got1[t]
        second_copy(t).start()

    def join_second(t):
        second_copy(t).wait_recv()
        part[t, 0] += got2[t, 1]
        third_copy(t).start()
        part[t, 1] += got2[t, 0]
        deal(t)

    def join_third(t):
        third_copy(t).wait_recv()
        part[t, 0] += got1[t, 0]
        deal(t)

    def project(j):
        def arrived(s, carry):
            for o in range(1, G):
                deal_arrival(j * nsub + s, o).wait_recv()
            return carry

        lax.fori_loop(0, nsub, arrived, 0)
        slot = lax.rem(j, slots)

        @pl.when(j >= slots)
        def _():
            load_states(j).wait()

        rows_at_once = 1024
        for k in range(kd):
            high, low = split(jnp.concatenate([tk[j, 2 * k], tk[j, 2 * k + 1]], axis=1))

            def bands(b, carry):
                rows = pl.ds(pl.multiple_of(b * rows_at_once, rows_at_once), rows_at_once)

                def times(side):
                    big, small = wide[k, side, rows, :], fine[k, side, rows, :]
                    return (
                        jnp.dot(big, high, preferred_element_type=F32)
                        + jnp.dot(big, low, preferred_element_type=F32)
                        + jnp.dot(small, high, preferred_element_type=F32)
                    )

                left, right = st[slot, 0, k, rows, :], st[slot, 1, k, rows, :]
                minus, plus = left - right, left + right
                over, under = times(0), times(1)
                acc[k, 0, rows, :] += over[:, :LANES] * minus + under[:, :LANES] * plus
                acc[k, 1, rows, :] += over[:, LANES:] * minus + under[:, LANES:] * plus
                return carry

            lax.fori_loop(0, NB // rows_at_once, bands, 0)

        @pl.when(j + slots < nch)
        def _():
            load_states(j + slots).start()

    def to_row(value):
        return jnp.sum(value.T, axis=0, keepdims=True)

    def prepare():
        for j in range(slots):
            load_states(j).wait()
        for k in range(kd):

            def bands(b, carry):
                rows = pl.ds(pl.multiple_of(b * LANES, LANES), LANES)
                total = jnp.zeros((LANES, LANES), F32)
                for q in range(nbc):
                    for side in range(2):
                        value = st[q, side, k, rows, :]
                        high, low = split(value)
                        wide[k, side, rows, q * LANES : (q + 1) * LANES] = high
                        fine[k, side, rows, q * LANES : (q + 1) * LANES] = low
                        total = total + value * value
                acc[k, 0, rows, :] = jnp.zeros((LANES, LANES), F32)
                acc[k, 1, rows, :] = jnp.zeros((LANES, LANES), F32)
                sums[x, pl.ds(2 * kd + k, 1), rows] = to_row(total)
                return carry

            lax.fori_loop(0, NB // LANES, bands, 0)

    load_turned(0).wait()
    load_own(0).wait()
    for h in range(nbc):
        produce(0, h)
        for t in range(h * batch, min(ahead, (h + 1) * batch)):
            share(t)
    reload(2)

    lag1, lag2, lag3 = LAGS
    lag = jnp.where(outer, lag3 + 1, lag2 + 1)

    def step(t, carry):
        @pl.when(t < nt)
        def _():
            expand(t)

        @pl.when(inner & (t >= lag1) & (t - lag1 < nt))
        def _():
            join_first(t - lag1)

        @pl.when(inner & (t >= lag2) & (t - lag2 < nt))
        def _():
            join_second(t - lag2)

        @pl.when(outer & (t >= lag3) & (t - lag3 < nt))
        def _():
            join_third(t - lag3)

        j = (t + ahead) // nsub

        @pl.when((t >= 0) & (lax.rem(t + ahead, nsub) == 0) & (j < nch))
        def _():
            @pl.when(j < nbc)
            def _():
                for q in range(1, nbc):

                    @pl.when(j == q)
                    def _():
                        load_turned(q).wait()

            @pl.when(j >= nbc)
            def _():
                turned_arrival(j).wait_recv()

            load_own(j).wait()
            for h in range(nbc):
                produce(j, h)
            reload(j + 2)

        @pl.when(t + ahead < nt)
        def _():
            share(t + ahead)

        for q in range(1, nbc):

            @pl.when(t == q * nt // (2 * nbc) + SHIFT)
            def _():
                for o in range(1, X):
                    turned_copy(o, q - 1).wait_send()
                    turned_copy(o, q).start()

        @pl.when(t == 2)
        def _():
            prepare()

        done = t - lag

        @pl.when((done >= 0) & (done < nt) & (lax.rem(done + nsub, nsub) == nsub - 1))
        def _():
            project(done // nsub)

        return carry

    lax.fori_loop(0, nt + lag3 + 1, step, 0)

    for k in range(kd):
        for m in range(2):

            for b in range(NB // LANES):
                rows = pl.ds(b * LANES, LANES)
                sums[x, pl.ds(m * kd + k, 1), rows] = to_row(acc[k, m, rows, :])

    def sum_copy(o):
        to = lax.rem(x + o, X)
        return remote(sums.at[x], sums.at[x], es.at[o - 1], er.at[o - 1], {"row": row, "rows": to})

    def sum_arrival(o):
        source = lax.rem(x - o + X, X)
        return remote(sums.at[source], sums.at[source], es.at[o - 1], er.at[o - 1], {"row": row, "rows": source})

    for o in range(1, X):
        sum_copy(o).start()
    for o in range(1, X):
        sum_arrival(o).wait_recv()
    total = sums[0]
    for o in range(1, X):
        total = total + sums[o]
    out_ref[...] = total

    for o in range(1, X):
        turned_copy(o, nbc - 1).wait_send()
    for o in range(1, X):
        sum_copy(o).wait_send()

    def settle(t, carry):
        for o in range(1, G):
            share_copy(t, o).wait_send()
            deal_copy(t, o).wait_send()

        @pl.when(outer & (t >= nt - flight))
        def _():
            first_copy(t).wait_send()

        @pl.when(inner)
        def _():
            second_copy(t).wait_send()
            third_copy(t).wait_send()

        return carry

    lax.fori_loop(0, nt, settle, 0)


def fits(row, X, hopping, states):
    per, nb, columns = hopping.shape[1:]
    kd, bands = states.shape[1:3]
    if row % LINE or nb % LANES or X < 2 or columns != X * nb:
        return False
    group = row // LINE
    nbc, span = nb // LANES, group * SUB
    return group > 1 and nbc >= 2 and LANES % span == 0 and bands % 256 == 0


def one_kernel(hopping, lattice, kgrid, tangent, states):
    X, G = lax.axis_size("rows"), lax.axis_size("row") // LINE
    per, nb = hopping.shape[1:3]
    kd, NB = states.shape[1:3]
    nbc = nb // LANES
    nch = X * nbc
    nt = nch * nb // (G * SUB)
    kb = 2 * kgrid.shape[1] // LINE
    cols = 2 * G * per
    slots = nbc
    tile = (SUB, LANES)
    dma = pltpu.SemaphoreType.DMA
    vmem = pl.BlockSpec(memory_space=pltpu.VMEM)
    hbm = pl.BlockSpec(memory_space=pl.ANY)
    rows_of_sums = -(-3 * kd // 8) * 8
    total = pl.pallas_call(
        functools.partial(kernel, (X, G, per, nb, kd, NB)),
        out_shape=jax.ShapeDtypeStruct((rows_of_sums, NB), F32),
        in_specs=[vmem, vmem, vmem, hbm, hbm],
        out_specs=vmem,
        scratch_shapes=[
            pltpu.VMEM((LINE * kb, 3 * cols), BF16),
            pltpu.VMEM((2, 2, per, nb, LANES), F32),
            pltpu.VMEM((nch, 2, per, LANES, nb), F32),
            pltpu.VMEM((nt, G, 2 * per, *tile), F32),
            pltpu.VMEM((nt, G, 2 * per, *tile), F32),
            pltpu.VMEM((nt, LINE, kb, *tile), F32),
            pltpu.VMEM((nt, LINE - 1, kb, *tile), F32),
            pltpu.VMEM((nt, LINE // 2, kb, *tile), F32),
            pltpu.VMEM((nch, 2 * kd, nb, LANES), F32),
            pltpu.VMEM((slots, 2, kd, NB, LANES), F32),
            pltpu.VMEM((kd, 2, NB, nb), BF16),
            pltpu.VMEM((kd, 2, NB, nb), BF16),
            pltpu.VMEM((kd, 2, NB, LANES), F32),
            pltpu.VMEM((X, rows_of_sums, NB), F32),
            dma((2,)),
            dma((nbc,)),
            dma((slots,)),
            dma(((X - 1) * nbc,)),
            dma(((X - 1) * nbc,)),
            dma((nt, G - 1)),
            dma((nt, G - 1)),
            dma((nt,)),
            dma((nt,)),
            dma((nt,)),
            dma((nt,)),
            dma((nt,)),
            dma((nt,)),
            dma((nt, G - 1)),
            dma((nt, G - 1)),
            dma((X - 1,)),
            dma((X - 1,)),
        ],
        compiler_params=pltpu.CompilerParams(
            collective_id=0, has_side_effects=True, vmem_limit_bytes=67043328
        ),
    )(lattice, kgrid, tangent, hopping, states)
    norm = total[2 * kd : 3 * kd]
    return total[: kd] / norm, total[kd : 2 * kd] / norm


def phases(kgrid, lattice, tangent):
    turns = jnp.mod(jnp.sum(kgrid[:, :, None] * lattice[:, None, :], axis=0), KGRID)
    angle = turns.astype(jnp.float32) * (2.0 * math.pi / KGRID)
    weight = jnp.sum(tangent[:, :, None] * lattice[:, None, :].astype(jnp.float32), axis=0)
    return (jnp.cos(angle), jnp.sin(angle), weight)


def project(m_re, m_im, rows, cols):
    high = lax.Precision.HIGH
    y_re = jnp.einsum("kmac,kic->kmai", m_re, cols[0], precision=high) - jnp.einsum(
        "kmac,kic->kmai", m_im, cols[1], precision=high
    )
    y_im = jnp.einsum("kmac,kic->kmai", m_re, cols[1], precision=high) + jnp.einsum(
        "kmac,kic->kmai", m_im, cols[0], precision=high
    )
    a = jnp.swapaxes(rows[0], 1, 2)[:, None]
    b = jnp.swapaxes(rows[1], 1, 2)[:, None]
    return jnp.sum(a * y_re + b * y_im, axis=2)


def exchanges(hopping, lattice, kgrid, tangent, states):
    row_count = hopping.shape[2]
    row_start = lax.axis_index("rows") * row_count
    state_rows = lax.dynamic_slice_in_dim(states, row_start, row_count, 3)
    cosine, sine, weight = phases(kgrid, lattice, tangent)
    first_d, second_d = -weight * sine, weight * cosine
    coef = jnp.stack(
        [
            jnp.stack([cosine, -sine], axis=1),
            jnp.stack([sine, cosine], axis=1),
            jnp.stack([first_d, -second_d], axis=1),
            jnp.stack([second_d, first_d], axis=1),
        ],
        axis=1,
    )
    halves = 2 if row_count % (2 * lax.axis_size("row")) == 0 else 1
    part = row_count // halves
    slabs = [
        lax.all_to_all(hopping[:, :, h * part : (h + 1) * part], "row", 2, 1, tiled=True)
        for h in range(halves)
    ]
    tiles = []
    for slab in slabs:
        blocks = jnp.einsum("kmpr,prac->kmac", coef, slab, precision=lax.Precision.HIGHEST)
        tiles.append(lax.all_to_all(blocks, "row", 0, 2, tiled=True))
    pieces = 0.0
    for h, tile in enumerate(tiles):
        rows = state_rows[..., h * part : (h + 1) * part]
        pieces = pieces + project(tile[:, 0::2], tile[:, 1::2], rows, states)
    totals = lax.psum(pieces, "rows")
    norm = jnp.sum(states[0] * states[0] + states[1] * states[1], axis=-1)
    return (totals[:, 0] / norm, totals[:, 1] / norm)


def per_device(hopping, lattice, kgrid, tangent, states):
    if fits(lax.axis_size("row"), lax.axis_size("rows"), hopping, states):
        return one_kernel(hopping, lattice, kgrid, tangent, states)
    return exchanges(hopping, lattice, kgrid, tangent, states)


def solution(mesh):
    placed = (P(None, "row", "rows", None), P(), P(), P(), P(None, "row", None, None))
    return jax.shard_map(
        per_device,
        mesh=mesh,
        in_specs=placed,
        out_specs=(P("row", None), P("row", None)),
        check_vma=False,
    )
```

```python
import functools
import math

import jax
import jax.numpy as jnp
from jax import lax
from jax.experimental import pallas as pl
from jax.experimental.pallas import tpu as pltpu
from jax.sharding import PartitionSpec as P

KGRID = 8
AHEAD = 2
FLIGHT = 3
LATE = 4
LAGS = (1, 3, 8)
SHIFT = 1
LINE = 4
LANES = 128
SUB = 8
MESH = pl.DeviceIdType.MESH
F32 = jnp.float32
BF16 = jnp.bfloat16


def split(value):
    high = value.astype(BF16)
    return high, (value - high.astype(F32)).astype(BF16)


def coefficients(lattice, kgrid, tangent, place, shape, per):
    exact = lax.Precision.HIGHEST
    block = shape[0] // LINE
    count = shape[1] // 2

    def iota(dims, axis):
        return lax.broadcasted_iota(jnp.int32, dims, axis)

    row = iota((shape[0], kgrid.shape[1]), 0)
    home = lax.div(row, block)
    home = jnp.where(place < LINE // 2, home, LINE - 1 - home)
    which = home * (block // 2) + lax.div(lax.rem(row, block), 2)
    pick_k = (which == iota(row.shape, 1)).astype(F32)
    column = iota((lattice.shape[1], shape[1]), 1)
    which = place * count + lax.div(column, 2 * per) * per + lax.rem(column, per)
    pick_r = (which == iota(column.shape, 0)).astype(F32)
    far = jnp.dot(lattice.astype(F32), pick_r, precision=exact, preferred_element_type=F32)

    def near(value):
        return lax.dot_general(pick_k, value, (((1,), (1,)), ((), ())), precision=exact, preferred_element_type=F32)

    def inner(left):
        return left[:, 0:1] * far[0:1] + left[:, 1:2] * far[1:2] + left[:, 2:3] * far[2:3]

    turns = inner(near(kgrid.astype(F32))).astype(jnp.int32) & (KGRID - 1)
    weight = inner(near(tangent))

    def wave(turn):
        turn = turn & (KGRID - 1)
        turn = jnp.minimum(turn, KGRID - turn)
        value = jnp.full(shape, -1.0, F32)
        for step in range(KGRID // 2):
            value = jnp.where(turn == step, F32(math.cos(2.0 * math.pi * step / KGRID)), value)
        return value

    cosine, sine = wave(turns), wave(turns - KGRID // 4)
    plus, minus = 0.5 * (cosine + sine), 0.5 * (cosine - sine)
    second = lax.rem(lax.div(iota(shape, 1), per), 2) == 1
    slope = lax.rem(iota(shape, 0), 2) == 1
    return jnp.where(slope, weight * jnp.where(second, -plus, minus), jnp.where(second, minus, plus))


def kernel(
    dims,
    lattice_ref,
    kgrid_ref,
    tangent_ref,
    hop,
    states,
    out_ref,
    coef3,
    hown,
    ht,
    uvs,
    uva,
    part,
    got1,
    got2,
    tk,
    st,
    wide,
    fine,
    acc,
    sums,
    hsem,
    tsem,
    ssem,
    xs,
    xr,
    gs,
    gr,
    s1,
    r1,
    s2,
    r2,
    s3,
    r3,
    ds,
    dr,
    es,
    er,
    s0,
    r0,
):
    X, G, per, nb, kd, NB = dims
    nbc = nb // LANES
    nch = X * nbc
    span = G * SUB
    nsub = nb // span
    nt = nch * nsub
    ahead, flight = min(AHEAD, nsub), FLIGHT
    kb = part.shape[2]
    slots = st.shape[0]
    row, x = lax.axis_index("row"), lax.axis_index("rows")
    a, g = row // G, lax.rem(row, G)
    outer = (a == 0) | (a == LINE - 1)
    inner = jnp.logical_not(outer)
    beside = a + 1 - 2 * lax.rem(a, 2)
    across = LINE - 1 - a
    own = jnp.where(outer, 0, 1)

    def column(j):
        home = lax.rem(x + j // nbc, X)
        return pl.multiple_of(home * nb + lax.rem(j, nbc) * LANES, LANES)

    def at(position, member):
        return {"row": position * G + member, "rows": x}

    def remote(src, dst, send, recv, device):
        return pltpu.make_async_remote_copy(
            src_ref=src, dst_ref=dst, send_sem=send, recv_sem=recv, device_id=device, device_id_type=MESH
        )

    def load_own(j):
        slot = lax.rem(j, 2)
        return pltpu.make_async_copy(hop.at[:, :, :, pl.ds(column(j), LANES)], hown.at[slot], hsem.at[slot])

    def load_turned(j):
        start = pl.multiple_of(x * nb, LANES)
        return pltpu.make_async_copy(
            hop.at[:, :, pl.ds(j * LANES, LANES), pl.ds(start, nb)], ht.at[j], tsem.at[j]
        )

    def load_states(j):
        slot = lax.rem(j, slots)
        return pltpu.make_async_copy(states.at[:, :, :, pl.ds(column(j), LANES)], st.at[slot], ssem.at[slot])

    def turned_copy(o, q):
        to = lax.rem(x - o + X, X)
        start = pl.multiple_of(to * nb, LANES)
        n = (o - 1) * nbc + q
        return remote(
            hop.at[:, :, pl.ds(q * LANES, LANES), pl.ds(start, nb)],
            ht.at[o * nbc + q],
            xs.at[n],
            xr.at[n],
            {"row": row, "rows": to},
        )

    def turned_arrival(j):
        return remote(ht.at[j], ht.at[j], xs.at[j - nbc], xr.at[j - nbc], {"row": row, "rows": lax.rem(x + 1, X)})

    def share_copy(t, o):
        to = lax.rem(g + o, G)
        return remote(uvs.at[t, to], uva.at[t, g], gs.at[t, o - 1], gr.at[t, o - 1], at(a, to))

    def share_arrival(t, o):
        source = lax.rem(g - o + G, G)
        return remote(uvs.at[t, source], uva.at[t, source], gs.at[t, o - 1], gr.at[t, o - 1], at(a, source))

    def first_copy(t):
        return remote(part.at[t, pl.ds(2, 2)], got1.at[t, pl.ds(1, 2)], s1.at[t], r1.at[t], at(beside, g))

    def late_copy(t):
        return remote(part.at[t, 1], got1.at[t, 0], s0.at[t], r0.at[t], at(beside, g))

    def second_copy(t):
        return remote(part.at[t, pl.ds(2, 2)], got2.at[t], s2.at[t], r2.at[t], at(across, g))

    def third_copy(t):
        return remote(part.at[t, 0], got1.at[t, 0], s3.at[t], r3.at[t], at(beside, g))

    def place_of(t, member):
        return pl.multiple_of(lax.rem(t, nsub) * span + member * SUB, SUB)

    def deal_copy(t, o):
        to = lax.rem(g + o, G)
        return remote(
            part.at[t, own, pl.ds(to * 2 * kd, 2 * kd)],
            tk.at[t // nsub, :, pl.ds(place_of(t, g), SUB), :],
            ds.at[t, o - 1],
            dr.at[t, o - 1],
            at(a, to),
        )

    def deal_arrival(t, o):
        source = lax.rem(g - o + G, G)
        there = tk.at[t // nsub, :, pl.ds(place_of(t, source), SUB), :]
        return remote(there, there, ds.at[t, o - 1], dr.at[t, o - 1], at(a, source))

    load_turned(0).start()
    load_own(0).start()

    barrier = pltpu.get_barrier_semaphore()
    for o in range(1, X):
        pl.semaphore_signal(barrier, inc=1, device_id={"row": row, "rows": lax.rem(x + o, X)}, device_id_type=MESH)
    for o in range(1, G):
        pl.semaphore_signal(barrier, inc=1, device_id=at(a, lax.rem(g + o, G)), device_id_type=MESH)
    for o in range(1, LINE):
        pl.semaphore_signal(barrier, inc=1, device_id=at(lax.rem(a + o, LINE), g), device_id_type=MESH)
    shape = (coef3.shape[0], coef3.shape[1] // 3)
    high, low = split(coefficients(lattice_ref[...], kgrid_ref[...], tangent_ref[...], a, shape, per))
    coef3[...] = jnp.concatenate([high, high, low], axis=1)

    pl.semaphore_wait(barrier, X + G + LINE - 3)

    for o in range(1, X):
        turned_copy(o, 0).start()
    for j in range(1, nbc):
        load_turned(j).start()
    load_own(1).start()
    for j in range(slots):
        load_states(j).start()


    batch = LANES // span

    def produce(j, h):
        slot = lax.rem(j, 2)
        rows = pl.ds(h * LANES, LANES)
        first = j * nsub + h * batch

        def one(r, carry):
            u = hown[slot, 0, r, rows, :] - ht[j, 1, r, :, rows].T
            v = ht[j, 0, r, :, rows].T + hown[slot, 1, r, rows, :]
            for q in range(LANES // SUB):
                t, member = first + q // G, q % G
                uvs[t, member, r] = u[q * SUB : (q + 1) * SUB]
                uvs[t, member, per + r] = v[q * SUB : (q + 1) * SUB]
            return carry

        lax.fori_loop(0, per, one, 0)

    def share(t):
        for o in range(1, G):
            share_copy(t, o).start()
        uva[t, g] = uvs[t, g]

    def reload(j):
        @pl.when(j < nch)
        def _():
            load_own(j).start()

    def expand(t):
        for o in range(1, G):
            share_arrival(t, o).wait_recv()
        for h in range(SUB // 8):
            rows = pl.ds(h * 8, 8)
            data = uva[t, :, :, rows, :].reshape(G * 2 * per, 8, LANES)
            data = jnp.swapaxes(data, 0, 1)
            done = []
            for i in range(0, 8, 2):
                high, low = split(jnp.concatenate([data[i], data[i + 1]], axis=1))
                both = jnp.concatenate([high, low, high], axis=0)
                out = jnp.dot(coef3[...], both, preferred_element_type=F32)
                done += [out[:, :LANES], out[:, LANES:]]
            done = jnp.swapaxes(jnp.stack(done), 0, 1)
            part[t, :, :, rows, :] = done.reshape(LINE, kb, 8, LANES)

        @pl.when(outer)
        def _():
            @pl.when(t >= flight)
            def _():
                first_copy(t - flight).wait_send()

            first_copy(t).start()

    def deal(t):
        for o in range(1, G):
            deal_copy(t, o).start()
        tk[t // nsub, :, pl.ds(place_of(t, g), SUB), :] = part[t, own, pl.ds(g * 2 * kd, 2 * kd)]

    def join_first(t):
        first_copy(t).wait_recv()
        part[t, 2:4] += got1[t, 1:3]
        second_copy(t).start()

    def join_second(t):
        second_copy(t).wait_recv()
        part[t, 0] += got2[t, 1]
        third_copy(t).start()
        part[t, 1] += got2[t, 0]

    def send_late(t):
        @pl.when(t >= flight)
        def _():
            late_copy(t - flight).wait_send()

        late_copy(t).start()

    def join_late(t):
        late_copy(t).wait_recv()
        part[t, 1] += got1[t, 0]
        deal(t)

    def join_third(t):
        third_copy(t).wait_recv()
        part[t, 0] += got1[t, 0]
        deal(t)

    def project(j):
        def arrived(s, carry):
            for o in range(1, G):
                deal_arrival(j * nsub + s, o).wait_recv()
            return carry

        lax.fori_loop(0, nsub, arrived, 0)
        slot = lax.rem(j, slots)

        @pl.when(j >= slots)
        def _():
            load_states(j).wait()

        rows_at_once = 1024
        for k in range(kd):
            high, low = split(jnp.concatenate([tk[j, 2 * k], tk[j, 2 * k + 1]], axis=1))

            def bands(b, carry):
                rows = pl.ds(pl.multiple_of(b * rows_at_once, rows_at_once), rows_at_once)

                def times(side):
                    big, small = wide[k, side, rows, :], fine[k, side, rows, :]
                    return (
                        jnp.dot(big, high, preferred_element_type=F32)
                        + jnp.dot(big, low, preferred_element_type=F32)
                        + jnp.dot(small, high, preferred_element_type=F32)
                    )

                left, right = st[slot, 0, k, rows, :], st[slot, 1, k, rows, :]
                minus, plus = left - right, left + right
                over, under = times(0), times(1)
                acc[k, 0, rows, :] += over[:, :LANES] * minus + under[:, :LANES] * plus
                acc[k, 1, rows, :] += over[:, LANES:] * minus + under[:, LANES:] * plus
                return carry

            lax.fori_loop(0, NB // rows_at_once, bands, 0)

        @pl.when(j + slots < nch)
        def _():
            load_states(j + slots).start()

    def to_row(value):
        return jnp.sum(value.T, axis=0, keepdims=True)

    def prepare():
        for j in range(slots):
            load_states(j).wait()
        for k in range(kd):

            def bands(b, carry):
                rows = pl.ds(pl.multiple_of(b * LANES, LANES), LANES)
                total = jnp.zeros((LANES, LANES), F32)
                for q in range(nbc):
                    for side in range(2):
                        value = st[q, side, k, rows, :]
                        high, low = split(value)
                        wide[k, side, rows, q * LANES : (q + 1) * LANES] = high
                        fine[k, side, rows, q * LANES : (q + 1) * LANES] = low
                        total = total + value * value
                acc[k, 0, rows, :] = jnp.zeros((LANES, LANES), F32)
                acc[k, 1, rows, :] = jnp.zeros((LANES, LANES), F32)
                sums[x, pl.ds(2 * kd + k, 1), rows] = to_row(total)
                return carry

            lax.fori_loop(0, NB // LANES, bands, 0)

    load_turned(0).wait()
    load_own(0).wait()
    for h in range(nbc):
        produce(0, h)
        for t in range(h * batch, min(ahead, (h + 1) * batch)):
            share(t)
    reload(2)

    lag1, lag2, lag3 = LAGS
    lag4 = LATE + 2
    lag = jnp.where(outer, lag3, lag4) + 1

    def step(t, carry):
        @pl.when(t < nt)
        def _():
            expand(t)

        @pl.when(inner & (t >= lag1) & (t - lag1 < nt))
        def _():
            join_first(t - lag1)

        @pl.when(inner & (t >= lag2) & (t - lag2 < nt))
        def _():
            join_second(t - lag2)

        @pl.when(inner & (t >= lag4) & (t - lag4 < nt))
        def _():
            join_late(t - lag4)

        @pl.when(outer & (t >= LATE) & (t - LATE < nt))
        def _():
            send_late(t - LATE)

        @pl.when(outer & (t >= lag3) & (t - lag3 < nt))
        def _():
            join_third(t - lag3)

        j = (t + ahead) // nsub

        @pl.when((t >= 0) & (lax.rem(t + ahead, nsub) == 0) & (j < nch))
        def _():
            @pl.when(j < nbc)
            def _():
                for q in range(1, nbc):

                    @pl.when(j == q)
                    def _():
                        load_turned(q).wait()

            @pl.when(j >= nbc)
            def _():
                turned_arrival(j).wait_recv()

            load_own(j).wait()
            for h in range(nbc):
                produce(j, h)
            reload(j + 2)

        @pl.when(t + ahead < nt)
        def _():
            share(t + ahead)

        for q in range(1, nbc):

            @pl.when(t == q * nt // (2 * nbc) + SHIFT)
            def _():
                for o in range(1, X):
                    turned_copy(o, q - 1).wait_send()
                    turned_copy(o, q).start()

        @pl.when(t == 2)
        def _():
            prepare()

        done = t - lag

        @pl.when((done >= 0) & (done < nt) & (lax.rem(done + nsub, nsub) == nsub - 1))
        def _():
            project(done // nsub)

        return carry

    lax.fori_loop(0, nt + max(lag3, lag4) + 1, step, 0)

    for k in range(kd):
        for m in range(2):

            for b in range(NB // LANES):
                rows = pl.ds(b * LANES, LANES)
                sums[x, pl.ds(m * kd + k, 1), rows] = to_row(acc[k, m, rows, :])

    def sum_copy(o):
        to = lax.rem(x + o, X)
        return remote(sums.at[x], sums.at[x], es.at[o - 1], er.at[o - 1], {"row": row, "rows": to})

    def sum_arrival(o):
        source = lax.rem(x - o + X, X)
        return remote(sums.at[source], sums.at[source], es.at[o - 1], er.at[o - 1], {"row": row, "rows": source})

    for o in range(1, X):
        sum_copy(o).start()
    for o in range(1, X):
        sum_arrival(o).wait_recv()
    total = sums[0]
    for o in range(1, X):
        total = total + sums[o]
    out_ref[...] = total

    for o in range(1, X):
        turned_copy(o, nbc - 1).wait_send()
    for o in range(1, X):
        sum_copy(o).wait_send()

    def settle(t, carry):
        for o in range(1, G):
            share_copy(t, o).wait_send()
            deal_copy(t, o).wait_send()

        @pl.when(outer & (t >= nt - flight))
        def _():
            first_copy(t).wait_send()
            late_copy(t).wait_send()

        @pl.when(inner)
        def _():
            second_copy(t).wait_send()
            third_copy(t).wait_send()

        return carry

    lax.fori_loop(0, nt, settle, 0)


def fits(row, X, hopping, states):
    per, nb, columns = hopping.shape[1:]
    kd, bands = states.shape[1:3]
    if row % LINE or nb % LANES or X < 2 or columns != X * nb:
        return False
    group = row // LINE
    nbc, span = nb // LANES, group * SUB
    return group > 1 and nbc >= 2 and LANES % span == 0 and bands % 256 == 0


def one_kernel(hopping, lattice, kgrid, tangent, states):
    X, G = lax.axis_size("rows"), lax.axis_size("row") // LINE
    per, nb = hopping.shape[1:3]
    kd, NB = states.shape[1:3]
    nbc = nb // LANES
    nch = X * nbc
    nt = nch * nb // (G * SUB)
    kb = 2 * kgrid.shape[1] // LINE
    cols = 2 * G * per
    slots = nbc
    tile = (SUB, LANES)
    dma = pltpu.SemaphoreType.DMA
    vmem = pl.BlockSpec(memory_space=pltpu.VMEM)
    hbm = pl.BlockSpec(memory_space=pl.ANY)
    rows_of_sums = -(-3 * kd // 8) * 8
    total = pl.pallas_call(
        functools.partial(kernel, (X, G, per, nb, kd, NB)),
        out_shape=jax.ShapeDtypeStruct((rows_of_sums, NB), F32),
        in_specs=[vmem, vmem, vmem, hbm, hbm],
        out_specs=vmem,
        scratch_shapes=[
            pltpu.VMEM((LINE * kb, 3 * cols), BF16),
            pltpu.VMEM((2, 2, per, nb, LANES), F32),
            pltpu.VMEM((nch, 2, per, LANES, nb), F32),
            pltpu.VMEM((nt, G, 2 * per, *tile), F32),
            pltpu.VMEM((nt, G, 2 * per, *tile), F32),
            pltpu.VMEM((nt, LINE, kb, *tile), F32),
            pltpu.VMEM((nt, LINE - 1, kb, *tile), F32),
            pltpu.VMEM((nt, LINE // 2, kb, *tile), F32),
            pltpu.VMEM((nch, 2 * kd, nb, LANES), F32),
            pltpu.VMEM((slots, 2, kd, NB, LANES), F32),
            pltpu.VMEM((kd, 2, NB, nb), BF16),
            pltpu.VMEM((kd, 2, NB, nb), BF16),
            pltpu.VMEM((kd, 2, NB, LANES), F32),
            pltpu.VMEM((X, rows_of_sums, NB), F32),
            dma((2,)),
            dma((nbc,)),
            dma((slots,)),
            dma(((X - 1) * nbc,)),
            dma(((X - 1) * nbc,)),
            dma((nt, G - 1)),
            dma((nt, G - 1)),
            dma((nt,)),
            dma((nt,)),
            dma((nt,)),
            dma((nt,)),
            dma((nt,)),
            dma((nt,)),
            dma((nt, G - 1)),
            dma((nt, G - 1)),
            dma((X - 1,)),
            dma((X - 1,)),
            dma((nt,)),
            dma((nt,)),
        ],
        compiler_params=pltpu.CompilerParams(
            collective_id=0, has_side_effects=True, vmem_limit_bytes=67043328
        ),
    )(lattice, kgrid, tangent, hopping, states)
    norm = total[2 * kd : 3 * kd]
    return total[: kd] / norm, total[kd : 2 * kd] / norm


def phases(kgrid, lattice, tangent):
    turns = jnp.mod(jnp.sum(kgrid[:, :, None] * lattice[:, None, :], axis=0), KGRID)
    angle = turns.astype(jnp.float32) * (2.0 * math.pi / KGRID)
    weight = jnp.sum(tangent[:, :, None] * lattice[:, None, :].astype(jnp.float32), axis=0)
    return (jnp.cos(angle), jnp.sin(angle), weight)


def project(m_re, m_im, rows, cols):
    high = lax.Precision.HIGH
    y_re = jnp.einsum("kmac,kic->kmai", m_re, cols[0], precision=high) - jnp.einsum(
        "kmac,kic->kmai", m_im, cols[1], precision=high
    )
    y_im = jnp.einsum("kmac,kic->kmai", m_re, cols[1], precision=high) + jnp.einsum(
        "kmac,kic->kmai", m_im, cols[0], precision=high
    )
    a = jnp.swapaxes(rows[0], 1, 2)[:, None]
    b = jnp.swapaxes(rows[1], 1, 2)[:, None]
    return jnp.sum(a * y_re + b * y_im, axis=2)


def exchanges(hopping, lattice, kgrid, tangent, states):
    row_count = hopping.shape[2]
    row_start = lax.axis_index("rows") * row_count
    state_rows = lax.dynamic_slice_in_dim(states, row_start, row_count, 3)
    cosine, sine, weight = phases(kgrid, lattice, tangent)
    first_d, second_d = -weight * sine, weight * cosine
    coef = jnp.stack(
        [
            jnp.stack([cosine, -sine], axis=1),
            jnp.stack([sine, cosine], axis=1),
            jnp.stack([first_d, -second_d], axis=1),
            jnp.stack([second_d, first_d], axis=1),
        ],
        axis=1,
    )
    halves = 2 if row_count % (2 * lax.axis_size("row")) == 0 else 1
    part = row_count // halves
    slabs = [
        lax.all_to_all(hopping[:, :, h * part : (h + 1) * part], "row", 2, 1, tiled=True)
        for h in range(halves)
    ]
    tiles = []
    for slab in slabs:
        blocks = jnp.einsum("kmpr,prac->kmac", coef, slab, precision=lax.Precision.HIGHEST)
        tiles.append(lax.all_to_all(blocks, "row", 0, 2, tiled=True))
    pieces = 0.0
    for h, tile in enumerate(tiles):
        rows = state_rows[..., h * part : (h + 1) * part]
        pieces = pieces + project(tile[:, 0::2], tile[:, 1::2], rows, states)
    totals = lax.psum(pieces, "rows")
    norm = jnp.sum(states[0] * states[0] + states[1] * states[1], axis=-1)
    return (totals[:, 0] / norm, totals[:, 1] / norm)


def per_device(hopping, lattice, kgrid, tangent, states):
    if fits(lax.axis_size("row"), lax.axis_size("rows"), hopping, states):
        return one_kernel(hopping, lattice, kgrid, tangent, states)
    return exchanges(hopping, lattice, kgrid, tangent, states)


def solution(mesh):
    placed = (P(None, "row", "rows", None), P(), P(), P(), P(None, "row", None, None))
    return jax.shard_map(
        per_device,
        mesh=mesh,
        in_specs=placed,
        out_specs=(P("row", None), P("row", None)),
        check_vma=False,
    )
```
